32 devices in a mesh: row: 16 (over z, y, x), col: 2 (over core).
Axes of the slice: x: 2, y: 2, z: 4, core: 2. Of those that a mesh axis runs over, the one named last changes fastest.
Arguments:
- adj_tiles: bfloat16 [16, 2, 128, 128, 128], P('row', 'col'), may hold values from 0 to 1, as said below
- tile_rows: int32 [16, 2, 128], P('row', 'col'), may hold values from 0 to 1, as said below
- tile_cols: int32 [16, 2, 128], P('row', 'col'), may hold values from 0 to 15, as said below
- tile_count: int32 [16, 2], P('row', 'col'), may hold values from 1 to 128, as said below
- tile_depth: int32 [32, 128], P(('row', 'col')), may hold values from 1 to 7, as said below
- source_ids: int32 [128], replicated, may hold values from 0 to 4095
Outputs:
- path_sums: float32 [4096, 128], P(('row', 'col'))
- log_scales: float32 [6, 128], replicated
The draws below stay inside these ranges and needn't reach their ends.
Inputs may be any that keep to these rules, and one draw needn't show every extreme that they name: `adj_tiles`: every entry is 0 or 1. The live slots of a device are its first tile_count slots; at least one device holds 128 live slots. `tile_rows`: slots past a device's live count carry 0. `tile_cols`: slots past a device's live count carry 0. `tile_depth`: the value 6 + 1 marks a tile that takes path counts at every level.
All inputs are finite; a program needn't handle non-finite values.
Results may differ from the reference program's by a relative error of at most 0.0003.
Values may be sent and summed in bfloat16 or wider, within the bound.
A program may use at most 64 MiB of HBM per device.

```python
import jax
import jax.numpy as jnp
from jax import lax

TILE = 128
PANEL = 128
PIECE = 128
KMAX = 128
LEVELS = 6
VERTICES = 4096
VTILES = 32
DEST_TILES = 2
SRC_TILES = 16
N_ROW = 16
N_COL = 2


def tile_lists(key):
    grid_shape = (N_ROW, N_COL)
    light = jax.random.randint(jax.random.fold_in(key, 11), grid_shape, KMAX // 4, KMAX // 2 + 1)
    heavy = jax.random.randint(jax.random.fold_in(key, 12), grid_shape, 0, 4) == 0
    loaded = jax.random.randint(jax.random.fold_in(key, 13), grid_shape, 3 * KMAX // 4, KMAX + 1)
    counts = jnp.where(heavy, loaded, light)
    chosen = jax.random.randint(jax.random.fold_in(key, 14), (), 0, N_ROW * N_COL)
    device_ids = jnp.arange(N_ROW * N_COL, dtype=jnp.int32).reshape(grid_shape)
    counts = jnp.where(device_ids == chosen, KMAX, counts).astype(jnp.int32)
    slot_ids = jnp.arange(KMAX, dtype=jnp.int32)[None, None, :]
    live_slots = slot_ids < counts[:, :, None]
    dest_ids = jax.random.randint(jax.random.fold_in(key, 15), grid_shape + (KMAX,), 0, DEST_TILES)
    src_ids = jax.random.randint(jax.random.fold_in(key, 16), grid_shape + (KMAX,), 0, SRC_TILES)
    dest_ids = jnp.where(live_slots, dest_ids, 0).astype(jnp.int32)
    src_ids = jnp.where(live_slots, src_ids, 0).astype(jnp.int32)
    return (counts, dest_ids, src_ids)


def draw_adj_tiles(key, part):
    counts, dest_ids, src_ids = tile_lists(key)
    piece_tiles = PIECE // TILE
    row_index = jnp.arange(N_ROW, dtype=jnp.int32)[:, None, None]
    col_index = jnp.arange(N_COL, dtype=jnp.int32)[None, :, None]
    dest_global = (row_index * (N_COL * piece_tiles) + dest_ids).astype(jnp.int32)
    src_global = ((src_ids // piece_tiles * N_COL + col_index) * piece_tiles + src_ids % piece_tiles).astype(jnp.int32)
    log_weight = jax.random.uniform(jax.random.fold_in(key, 33), (VTILES, TILE), jnp.float32, jnp.log(0.3), jnp.log(1.0))
    vertex_weight = jnp.exp(log_weight)
    dest_weight = jnp.take(vertex_weight, dest_global, axis=0)
    src_weight = jnp.take(vertex_weight, src_global, axis=0)
    pair_weight = dest_weight[:, :, :, :, None] * src_weight[:, :, :, None, :]
    slot_shape = (N_ROW, N_COL, KMAX, 1, 1)
    log_density = jax.random.uniform(jax.random.fold_in(key, 31), slot_shape, jnp.float32, jnp.log(0.15), jnp.log(0.6))
    density = jnp.exp(log_density)
    offset = jax.random.randint(jax.random.fold_in(key, 34), slot_shape, 0, TILE)
    positions = jnp.arange(TILE, dtype=jnp.int32)
    spread = positions[None, :] - positions[:, None]
    inside = (spread[None, None, None, :, :] - offset) % TILE < TILE // 4
    rate = jnp.where(inside, jnp.minimum(1.0, 4.0 * density * pair_weight), 0.15 * pair_weight)
    coins = jax.random.uniform(jax.random.fold_in(key, 32), (N_ROW, N_COL, KMAX, TILE, TILE), jnp.float32)
    return (coins < rate).astype(jnp.float32).astype(jnp.bfloat16)


def draw_tile_count(key, part):
    return tile_lists(key)[0]


def draw_tile_rows(key, part):
    return tile_lists(key)[1]


def draw_tile_cols(key, part):
    return tile_lists(key)[2]


def draw_tile_depth(key, part):
    base_level = jax.random.randint(jax.random.fold_in(key, 21), (VTILES, 1), 0, LEVELS + 1)
    offset = jax.random.randint(jax.random.fold_in(key, 22), (VTILES, PANEL), 0, LEVELS + 1)
    return (1 + jnp.maximum(base_level, offset)).astype(jnp.int32)


def place_ends(values, own_key, low, largest):
    longest = values.shape.index(max(values.shape))
    spots = []
    for shift in (0, 1):
        where = [jax.random.randint(jax.random.fold_in(own_key, axis), (), 0, length) for axis, length in enumerate(values.shape)]
        where[longest] = (where[longest] + shift) % values.shape[longest]
        spots.append(tuple(where))
    return values.at[spots[0]].set(low).at[spots[1]].set(largest)


def setup_inputs(seed: int = 0) -> dict:
    keys = jax.random.split(jax.random.key(seed), 7)
    adj_tiles = draw_adj_tiles(jax.random.fold_in(keys[6], 71), 0)
    tile_rows = draw_tile_rows(jax.random.fold_in(keys[6], 71), 0)
    tile_cols = draw_tile_cols(jax.random.fold_in(keys[6], 71), 0)
    tile_count = draw_tile_count(jax.random.fold_in(keys[6], 71), 0)
    tile_depth = draw_tile_depth(jax.random.fold_in(keys[6], 71), 0)
    source_ids = place_ends(jax.random.randint(keys[5], (PANEL,), 0, VERTICES), jax.random.fold_in(keys[5], 1), 0, VERTICES - 1).astype(jnp.int32)
    return dict(adj_tiles=adj_tiles, tile_rows=tile_rows, tile_cols=tile_cols, tile_count=tile_count, tile_depth=tile_depth, source_ids=source_ids)


EPSILON = 1e-06

def reference(adj_tiles, tile_rows, tile_cols, tile_count, tile_depth, source_ids):
    piece_tiles = PIECE // TILE
    tile_total = VERTICES // TILE
    row_slots = N_COL * KMAX
    slot_ids = jnp.arange(KMAX, dtype=jnp.int32)[None, None, :]
    row_index = jnp.arange(N_ROW, dtype=jnp.int32)[:, None, None]
    col_index = jnp.arange(N_COL, dtype=jnp.int32)[None, :, None]
    dest_tile = (row_index * (N_COL * piece_tiles) + tile_rows).reshape(-1).astype(jnp.int32)
    src_tile = ((tile_cols // piece_tiles * N_COL + col_index) * piece_tiles + tile_cols % piece_tiles).reshape(-1).astype(jnp.int32)
    live_slots = (slot_ids < tile_count[:, :, None]).astype(jnp.float32).reshape(-1)
    flat_tiles = adj_tiles.reshape(N_ROW * row_slots, TILE, TILE)

    def product(frontier):

        def one_row(summed, row_number):
            first_slot = (row_number * row_slots).astype(jnp.int32)
            block_part = lax.dynamic_slice_in_dim(flat_tiles, first_slot, row_slots, 0).astype(jnp.float32)
            dest_part = lax.dynamic_slice_in_dim(dest_tile, first_slot, row_slots, 0)
            src_part = lax.dynamic_slice_in_dim(src_tile, first_slot, row_slots, 0)
            weights = lax.dynamic_slice_in_dim(live_slots, first_slot, row_slots, 0)
            picked = jnp.take(frontier, src_part, axis=0).astype(jnp.float32)
            slot_terms = jnp.einsum('kij,kjs->kis', block_part, picked, precision=lax.Precision.HIGHEST)
            slot_terms = slot_terms * weights[:, None, None]
            return (summed.at[dest_part].add(slot_terms), None)
        zero_sums = jnp.zeros((tile_total, TILE, PANEL), jnp.float32)
        summed, unused = lax.scan(one_row, zero_sums, jnp.arange(N_ROW, dtype=jnp.int32))
        return summed
    vertex_ids = jnp.arange(VERTICES, dtype=jnp.int32)
    start_panel = (vertex_ids[:, None] == source_ids[None, :]).astype(jnp.float32)
    path_sums = start_panel
    frontier = start_panel.astype(jnp.bfloat16)
    log_scales = []
    for level_index in range(1, LEVELS + 1):
        summed = product(frontier.reshape(tile_total, TILE, PANEL))
        reached = (tile_depth >= level_index).astype(jnp.float32)
        raw_paths = (summed * reached[:, None, :]).reshape(VERTICES, PANEL)
        mean_square = lax.optimization_barrier(jnp.sum(raw_paths * raw_paths, axis=0)) / VERTICES + EPSILON
        scaled = raw_paths * lax.rsqrt(mean_square)
        path_sums = path_sums + scaled
        log_scales.append(0.5 * jnp.log(mean_square))
        frontier = scaled.astype(jnp.bfloat16)
    return (path_sums, jnp.stack(log_scales))
```

```python
import functools
import math

import jax
import jax.numpy as jnp
from jax import lax
from jax.experimental import pallas as pl
from jax.experimental.pallas import tpu as pltpu
from jax.sharding import PartitionSpec as P

TILE = 128
LEVELS = 6
EPSILON = 1e-06
CHUNK = 16
MESH = pl.DeviceIdType.MESH


def build_kernel(count_ref, rows_ref, cols_ref, adj_ref, dense_ref, blocks, sems):
    slots = adj_ref.shape[0]
    chunk = math.gcd(CHUNK, slots)
    count = count_ref[0]

    def fetch(index):
        return pltpu.make_async_copy(
            adj_ref.at[pl.ds(index * chunk, chunk)], blocks.at[pl.ds(index * chunk, chunk)], sems.at[index]
        )

    for index in range(slots // chunk):
        @pl.when(index * chunk < count)
        def _():
            fetch(index).start()

    dense_ref[...] = jnp.zeros_like(dense_ref)

    for index in range(slots // chunk):
        @pl.when(index * chunk < count)
        def _():
            fetch(index).wait()

            def add(slot, carry):
                row = pl.multiple_of(rows_ref[slot] * TILE, TILE)
                col = pl.multiple_of(cols_ref[slot] * TILE, TILE)
                where = (pl.ds(row, TILE), pl.ds(col, TILE))
                dense_ref[where] = dense_ref[where] + blocks[slot]
                return carry

            lax.fori_loop(index * chunk, jnp.minimum(count, (index + 1) * chunk), add, 0)


def build(adj, rows, cols, count, dest_tiles, src_tiles):
    slots = adj.shape[0]
    smem = pl.BlockSpec(memory_space=pltpu.SMEM)
    return pl.pallas_call(
        build_kernel,
        out_shape=jax.ShapeDtypeStruct((dest_tiles * TILE, src_tiles * TILE), adj.dtype),
        in_specs=[smem, smem, smem, pl.BlockSpec(memory_space=pl.ANY)],
        out_specs=pl.BlockSpec(memory_space=pltpu.VMEM),
        scratch_shapes=[
            pltpu.VMEM(adj.shape, adj.dtype),
            pltpu.SemaphoreType.DMA((slots // math.gcd(CHUNK, slots),)),
        ],
        compiler_params=pltpu.CompilerParams(vmem_limit_bytes=40 * 1024 * 1024),
        name="build_dense",
    )(count, rows, cols, adj)


def level_kernel(
    row_total, col_total, inner,
    dense_ref, depth_ref, source_ref, sums_ref, logs_ref,
    panel, partial, squares, raw, depths,
    panel_send, panel_recv, part_send, part_recv, square_send, square_recv, depth_send, depth_recv,
):
    me_row, me_col = lax.axis_index("row"), lax.axis_index("col")
    piece = sums_ref.shape[0]
    piece_tiles = depth_ref.shape[0]
    half = piece // 2
    vertex_total = piece * row_total * col_total
    outer = row_total // inner
    my_inner, my_outer = lax.rem(me_row, inner), lax.div(me_row, inner)
    row_peers = [lax.rem(me_row + step, row_total) for step in range(1, row_total)]
    col_peers = [lax.rem(me_col + step, col_total) for step in range(1, col_total)]
    inner_peers = [lax.rem(my_inner + step, inner) for step in range(1, inner)]
    outer_peers = [lax.rem(my_outer + step, outer) for step in range(1, outer)]

    barrier = pltpu.get_barrier_semaphore()
    for peer in row_peers:
        pl.semaphore_signal(barrier, inc=1, device_id=(peer, me_col), device_id_type=MESH)
    for peer in col_peers:
        pl.semaphore_signal(barrier, inc=1, device_id=(me_row, peer), device_id_type=MESH)

    sources = source_ref[...]
    offsets = lax.broadcasted_iota(jnp.int32, (piece, sources.shape[1]), 0)
    for row in range(row_total):
        first = (row * col_total + me_col) * piece
        panel[0, row] = (offsets + first == sources).astype(jnp.float32).astype(panel.dtype)
    mine = (offsets + (me_row * col_total + me_col) * piece == sources).astype(jnp.float32)
    sums_ref[...] = mine
    depths[pl.ds(me_col, 1)] = depth_ref[...][None]

    def product(slot):
        whole = panel[slot].reshape(row_total * piece, panel.shape[3])
        return jnp.dot(dense_ref[...], whole, preferred_element_type=jnp.float32)

    def copies(source, target, send, recv, peers):
        return [
            pltpu.make_async_remote_copy(
                src_ref=source, dst_ref=target, send_sem=send(step), recv_sem=recv,
                device_id=peer, device_id_type=MESH,
            )
            for step, peer in enumerate(peers)
        ]

    def arrival(target, recv):
        return pltpu.make_async_copy(target, target, recv)

    def total_square(slot):
        mean_square = jnp.sum(squares[slot], axis=0) / vertex_total + EPSILON
        return mean_square

    panel_sends, square_sends, part_sends, depth_sends = [], [], [], []
    scale = None
    for level in range(1, LEVELS + 1):
        slot = level % 2
        before = (level + 1) % 2
        if level > 1:
            for group_step, peer in enumerate(inner_peers):
                owner = my_outer * inner + peer
                place = panel.at[before, owner, pl.ds(0, half)]
                arrival(place, panel_recv.at[before, owner, 0]).wait()
                base = inner - 1 + (group_step + 1) * (outer - 1)
                sends = copies(
                    place, place, lambda step: panel_send.at[0, base + step], panel_recv.at[before, owner, 0],
                    [(other * inner + my_inner, me_col) for other in outer_peers],
                )
                for copy in sends:
                    copy.start()
                panel_sends += sends
            for group_step, peer in enumerate(outer_peers):
                owner = peer * inner + my_inner
                place = panel.at[before, owner, pl.ds(half, piece - half)]
                arrival(place, panel_recv.at[before, owner, 1]).wait()
                base = outer - 1 + (group_step + 1) * (inner - 1)
                sends = copies(
                    place, place, lambda step: panel_send.at[1, base + step], panel_recv.at[before, owner, 1],
                    [(my_outer * inner + other, me_col) for other in inner_peers],
                )
                for copy in sends:
                    copy.start()
                panel_sends += sends
            for peer_outer in outer_peers:
                for peer_inner in [my_inner] + inner_peers:
                    owner = peer_outer * inner + peer_inner
                    place = panel.at[before, owner, pl.ds(0, half)]
                    arrival(place, panel_recv.at[before, owner, 0]).wait()
            for peer_inner in inner_peers:
                for peer_outer in [my_outer] + outer_peers:
                    owner = peer_outer * inner + peer_inner
                    place = panel.at[before, owner, pl.ds(half, piece - half)]
                    arrival(place, panel_recv.at[before, owner, 1]).wait()
        partial[slot, pl.ds(me_col, 1)] = product(before)[None]
        if level == 1:
            pl.semaphore_wait(barrier, row_total + col_total - 2)
            depth_sends = copies(
                depth_ref, depths.at[me_col], lambda step: depth_send.at[step], depth_recv.at[me_col],
                [(me_row, peer) for peer in col_peers],
            )
            for copy in depth_sends:
                copy.start()
        for copy in part_sends:
            copy.wait_send()
        part_sends = copies(
            partial.at[slot, me_col], partial.at[slot, me_col],
            lambda step: part_send.at[step], part_recv.at[slot, me_col],
            [(me_row, peer) for peer in col_peers],
        )
        for copy in part_sends:
            copy.start()
        for copy in panel_sends + square_sends:
            copy.wait_send()
        panel_sends, square_sends = [], []
        if level > 1:
            for peer in row_peers:
                arrival(squares.at[before, peer], square_recv.at[before, peer]).wait()
            mean_square = total_square(before)
            scale = lax.rsqrt(mean_square)
            logs_ref[level - 2 : level - 1] = 0.5 * jnp.log(mean_square)
            sums_ref[...] = sums_ref[...] + raw[me_col] * scale
        for peer in col_peers:
            arrival(partial.at[slot, peer], part_recv.at[slot, peer]).wait()
            if level == 1:
                arrival(depths.at[peer], depth_recv.at[peer]).wait()
        summed = partial[slot, 0]
        for col in range(1, col_total):
            summed = summed + partial[slot, col]
        reached = (depths[...] >= level).astype(jnp.float32)
        if level > 1:
            reached = reached * scale
        tiles = summed.reshape(col_total * piece_tiles, TILE, summed.shape[1])
        tiles = tiles * reached.reshape(col_total * piece_tiles, 1, summed.shape[1])
        raw[...] = tiles.reshape(raw.shape)
        if level < LEVELS:
            panel[slot, pl.ds(me_row, 1)] = raw[pl.ds(me_col, 1)].astype(panel.dtype)
            place = panel.at[slot, me_row, pl.ds(0, half)]
            panel_sends += copies(
                place, place, lambda step: panel_send.at[0, step], panel_recv.at[slot, me_row, 0],
                [(my_outer * inner + other, me_col) for other in inner_peers]
                + [(other * inner + my_inner, me_col) for other in outer_peers],
            )
            place = panel.at[slot, me_row, pl.ds(half, piece - half)]
            panel_sends += copies(
                place, place, lambda step: panel_send.at[1, step], panel_recv.at[slot, me_row, 1],
                [(other * inner + my_inner, me_col) for other in outer_peers]
                + [(my_outer * inner + other, me_col) for other in inner_peers],
            )
            for copy in panel_sends:
                copy.start()
        flat = tiles.reshape(col_total * piece, summed.shape[1])
        squares[slot, pl.ds(me_row, 1)] = jnp.sum(flat * flat, axis=0, keepdims=True)[None]
        square_sends = copies(
            squares.at[slot, me_row], squares.at[slot, me_row],
            lambda step: square_send.at[step], square_recv.at[slot, me_row],
            [(peer, me_col) for peer in row_peers],
        )
        for copy in square_sends:
            copy.start()
    last = LEVELS % 2
    for peer in row_peers:
        arrival(squares.at[last, peer], square_recv.at[last, peer]).wait()
    mean_square = total_square(last)
    logs_ref[LEVELS - 1 : LEVELS] = 0.5 * jnp.log(mean_square)
    sums_ref[...] = sums_ref[...] + raw[me_col] * lax.rsqrt(mean_square)
    for copy in part_sends + square_sends + depth_sends:
        copy.wait_send()


def inner_size(total):
    return max(size for size in range(1, total + 1) if total % size == 0 and size * size <= total)


def levels(dense, depth, source_ids, row_total, col_total):
    piece_tiles, width = depth.shape
    piece = piece_tiles * TILE
    inner = inner_size(row_total)
    vmem = pl.BlockSpec(memory_space=pltpu.VMEM)
    dma = pltpu.SemaphoreType.DMA
    return pl.pallas_call(
        functools.partial(level_kernel, row_total, col_total, inner),
        out_shape=(
            jax.ShapeDtypeStruct((piece, width), jnp.float32),
            jax.ShapeDtypeStruct((LEVELS, width), jnp.float32),
        ),
        in_specs=[vmem, vmem, vmem],
        out_specs=(vmem, vmem),
        scratch_shapes=[
            pltpu.VMEM((2, row_total, piece, width), jnp.bfloat16),
            pltpu.VMEM((2, col_total, col_total * piece, width), jnp.float32),
            pltpu.VMEM((2, row_total, 1, width), jnp.float32),
            pltpu.VMEM((col_total, piece, width), jnp.float32),
            pltpu.VMEM((col_total, piece_tiles, width), jnp.int32),
            dma((2, row_total)),
            dma((2, row_total, 2)),
            dma((col_total,)),
            dma((2, col_total)),
            dma((row_total,)),
            dma((2, row_total)),
            dma((col_total,)),
            dma((col_total,)),
        ],
        compiler_params=pltpu.CompilerParams(
            collective_id=0, has_side_effects=True, vmem_limit_bytes=56 * 1024 * 1024
        ),
        name="levels",
    )(dense, depth, source_ids)


def local(adj_tiles, tile_rows, tile_cols, tile_count, tile_depth, source_ids):
    row_total, col_total = lax.axis_size("row"), lax.axis_size("col")
    piece_tiles, width = tile_depth.shape
    dense = build(
        adj_tiles[0, 0], tile_rows[0, 0], tile_cols[0, 0], tile_count[0], col_total * piece_tiles, row_total * piece_tiles
    )
    return levels(dense, tile_depth, source_ids.reshape(1, width), row_total, col_total)


def solution(mesh):
    in_specs = (
        P("row", "col", None, None, None),
        P("row", "col", None),
        P("row", "col", None),
        P("row", "col"),
        P(("row", "col"), None),
        P(),
    )
    out_specs = (P(("row", "col"), None), P())
    return jax.shard_map(local, mesh=mesh, in_specs=in_specs, out_specs=out_specs, check_vma=False)
```

```python
import functools
import math

import jax
import jax.numpy as jnp
from jax import lax
from jax.experimental import pallas as pl
from jax.experimental.pallas import tpu as pltpu
from jax.sharding import PartitionSpec as P

TILE = 128
LEVELS = 6
EPSILON = 1e-06
CHUNK = 16
SPLIT_NUM = 4
MESH = pl.DeviceIdType.MESH


def build_kernel(count_ref, rows_hbm, cols_hbm, adj_ref, dense_ref, blocks, rows_ref, cols_ref, sems, list_sems):
    slots = adj_ref.shape[0]
    chunk = math.gcd(CHUNK, slots)
    count = count_ref[0]

    def fetch(index):
        return pltpu.make_async_copy(
            adj_ref.at[pl.ds(index * chunk, chunk)], blocks.at[pl.ds(index * chunk, chunk)], sems.at[index]
        )

    lists = [
        pltpu.make_async_copy(rows_hbm, rows_ref, list_sems.at[0]),
        pltpu.make_async_copy(cols_hbm, cols_ref, list_sems.at[1]),
    ]
    for copy in lists:
        copy.start()
    for index in range(slots // chunk):
        @pl.when(index * chunk < count)
        def _():
            fetch(index).start()

    dense_ref[...] = jnp.zeros_like(dense_ref)
    for copy in lists:
        copy.wait()

    for index in range(slots // chunk):
        @pl.when(index * chunk < count)
        def _():
            fetch(index).wait()

            def add(slot, carry):
                row = pl.multiple_of(rows_ref[slot] * TILE, TILE)
                col = pl.multiple_of(cols_ref[slot] * TILE, TILE)
                where = (pl.ds(row, TILE), pl.ds(col, TILE))
                dense_ref[where] = dense_ref[where] + blocks[slot]
                return carry

            lax.fori_loop(index * chunk, jnp.minimum(count, (index + 1) * chunk), add, 0)


def build(adj, rows, cols, count, dest_tiles, src_tiles):
    slots = adj.shape[0]
    smem, hbm = pl.BlockSpec(memory_space=pltpu.SMEM), pl.BlockSpec(memory_space=pl.ANY)
    return pl.pallas_call(
        build_kernel,
        out_shape=jax.ShapeDtypeStruct((dest_tiles * TILE, src_tiles * TILE), adj.dtype),
        in_specs=[smem, hbm, hbm, hbm],
        out_specs=pl.BlockSpec(memory_space=pltpu.VMEM),
        scratch_shapes=[
            pltpu.VMEM(adj.shape, adj.dtype),
            pltpu.SMEM(rows.shape, rows.dtype),
            pltpu.SMEM(cols.shape, cols.dtype),
            pltpu.SemaphoreType.DMA((slots // math.gcd(CHUNK, slots),)),
            pltpu.SemaphoreType.DMA((2,)),
        ],
        compiler_params=pltpu.CompilerParams(vmem_limit_bytes=40 * 1024 * 1024),
        name="build_dense",
    )(count, rows, cols, adj)


def mirrored(me, size):
    if size & (size - 1):
        return [lax.rem(me + step, size) for step in range(1, size)]
    peers = []
    for step in range(1, size):
        peer = me
        for bit in range(size.bit_length()):
            if step >> bit & 1:
                peer = peer + (1 << bit) * (1 - 2 * lax.rem(lax.div(me, 1 << bit), 2))
        peers.append(peer)
    return peers


def level_kernel(
    row_total, col_total, inner,
    dense_hbm, depth_ref, source_ref, sums_ref, logs_ref,
    dense_ref, dense_sem, panel, partial, squares, raw, depths,
    panel_send, panel_recv, part_send, part_recv, square_send, square_recv, depth_send, depth_recv,
):
    me_row, me_col = lax.axis_index("row"), lax.axis_index("col")
    piece = sums_ref.shape[0]
    piece_tiles = depth_ref.shape[0]
    half = piece * SPLIT_NUM // 8
    vertex_total = piece * row_total * col_total
    outer = row_total // inner
    my_inner, my_outer = lax.rem(me_row, inner), lax.div(me_row, inner)
    row_peers = [lax.rem(me_row + step, row_total) for step in range(1, row_total)]
    col_peers = [lax.rem(me_col + step, col_total) for step in range(1, col_total)]
    inner_peers = mirrored(my_inner, inner)
    steps = sorted(range(1, outer), key=lambda step: min(step, outer - step))
    outer_peers = [lax.rem(my_outer + step, outer) for step in steps]

    dense_copy = pltpu.make_async_copy(dense_hbm, dense_ref, dense_sem)
    dense_copy.start()
    barrier = pltpu.get_barrier_semaphore()
    for peer in row_peers:
        pl.semaphore_signal(barrier, inc=1, device_id=(peer, me_col), device_id_type=MESH)
    for peer in col_peers:
        pl.semaphore_signal(barrier, inc=1, device_id=(me_row, peer), device_id_type=MESH)

    sources = source_ref[...]
    offsets = lax.broadcasted_iota(jnp.int32, (piece, sources.shape[1]), 0)
    for row in range(row_total):
        first = (row * col_total + me_col) * piece
        panel[0, row] = (offsets + first == sources).astype(jnp.float32).astype(panel.dtype)
    mine = (offsets + (me_row * col_total + me_col) * piece == sources).astype(jnp.float32)
    sums_ref[...] = mine
    depths[pl.ds(me_col, 1)] = depth_ref[...][None]

    def product(slot, group):
        span = inner * piece
        block = panel[slot, pl.ds(group * inner, inner)].reshape(span, panel.shape[3])
        columns = dense_ref[:, pl.ds(pl.multiple_of(group * span, span), span)]
        return jnp.dot(columns, block, preferred_element_type=jnp.float32)

    def copies(source, target, send, recv, peers):
        return [
            pltpu.make_async_remote_copy(
                src_ref=source, dst_ref=target, send_sem=send(step), recv_sem=recv,
                device_id=peer, device_id_type=MESH,
            )
            for step, peer in enumerate(peers)
        ]

    def arrival(target, recv):
        return pltpu.make_async_copy(target, target, recv)

    def total_square(slot):
        mean_square = jnp.sum(squares[slot], axis=0) / vertex_total + EPSILON
        return mean_square

    panel_sends, square_sends, part_sends, depth_sends = [], [], [], []
    scale = None
    for level in range(1, LEVELS + 1):
        slot = level % 2
        before = (level + 1) % 2
        if level > 1:
            turns = [(step, 0, peer) for step, peer in enumerate(inner_peers)]
            turns += [(step, 1, peer) for step, peer in enumerate(outer_peers)]
            for group_step, part_index, peer in sorted(turns, key=lambda turn: turn[:2]):
                if part_index == 0:
                    owner = my_outer * inner + peer
                    rows = pl.ds(0, half)
                    targets = [(other * inner + my_inner, me_col) for other in outer_peers]
                    base = inner - 1 + (group_step + 1) * (outer - 1)
                else:
                    owner = peer * inner + my_inner
                    rows = pl.ds(half, piece - half)
                    targets = [(my_outer * inner + other, me_col) for other in inner_peers]
                    base = outer - 1 + (group_step + 1) * (inner - 1)
                place = panel.at[before, owner, rows]
                arrival(place, panel_recv.at[before, owner, part_index]).wait()
                sends = copies(
                    place, place, lambda step: panel_send.at[part_index, base + step],
                    panel_recv.at[before, owner, part_index], targets,
                )
                for copy in sends:
                    copy.start()
                panel_sends += sends
        else:
            dense_copy.wait()
        total = None
        for group in [my_outer] + outer_peers:
            if level > 1:
                for peer_inner in [my_inner] + inner_peers:
                    owner = group * inner + peer_inner
                    if group is not my_outer:
                        arrival(panel.at[before, owner, pl.ds(0, half)], panel_recv.at[before, owner, 0]).wait()
                    if peer_inner is not my_inner:
                        place = panel.at[before, owner, pl.ds(half, piece - half)]
                        arrival(place, panel_recv.at[before, owner, 1]).wait()
            part = product(before, group)
            total = part if total is None else total + part
        partial[slot, pl.ds(me_col, 1)] = total[None]
        if level == 1:
            pl.semaphore_wait(barrier, row_total + col_total - 2)
            depth_sends = copies(
                depth_ref, depths.at[me_col], lambda step: depth_send.at[step], depth_recv.at[me_col],
                [(me_row, peer) for peer in col_peers],
            )
            for copy in depth_sends:
                copy.start()
        for copy in part_sends:
            copy.wait_send()
        part_sends = copies(
            partial.at[slot, me_col], partial.at[slot, me_col],
            lambda step: part_send.at[step], part_recv.at[slot, me_col],
            [(me_row, peer) for peer in col_peers],
        )
        for copy in part_sends:
            copy.start()
        for copy in panel_sends + square_sends:
            copy.wait_send()
        panel_sends, square_sends = [], []
        if level > 1:
            for peer in row_peers:
                arrival(squares.at[before, peer], square_recv.at[before, peer]).wait()
            mean_square = total_square(before)
            scale = lax.rsqrt(mean_square)
            logs_ref[level - 2 : level - 1] = 0.5 * jnp.log(mean_square)
            sums_ref[...] = sums_ref[...] + raw[me_col] * scale
        for peer in col_peers:
            arrival(partial.at[slot, peer], part_recv.at[slot, peer]).wait()
            if level == 1:
                arrival(depths.at[peer], depth_recv.at[peer]).wait()
        summed = partial[slot, 0]
        for col in range(1, col_total):
            summed = summed + partial[slot, col]
        reached = (depths[...] >= level).astype(jnp.float32)
        if level > 1:
            reached = reached * scale
        tiles = summed.reshape(col_total * piece_tiles, TILE, summed.shape[1])
        tiles = tiles * reached.reshape(col_total * piece_tiles, 1, summed.shape[1])
        raw[...] = tiles.reshape(raw.shape)
        if level < LEVELS:
            panel[slot, pl.ds(me_row, 1)] = raw[pl.ds(me_col, 1)].astype(panel.dtype)
            place = panel.at[slot, me_row, pl.ds(0, half)]
            panel_sends += copies(
                place, place, lambda step: panel_send.at[0, step], panel_recv.at[slot, me_row, 0],
                [(my_outer * inner + other, me_col) for other in inner_peers]
                + [(other * inner + my_inner, me_col) for other in outer_peers],
            )
            place = panel.at[slot, me_row, pl.ds(half, piece - half)]
            panel_sends += copies(
                place, place, lambda step: panel_send.at[1, step], panel_recv.at[slot, me_row, 1],
                [(other * inner + my_inner, me_col) for other in outer_peers]
                + [(my_outer * inner + other, me_col) for other in inner_peers],
            )
            for copy in panel_sends:
                copy.start()
        flat = tiles.reshape(col_total * piece, summed.shape[1])
        squares[slot, pl.ds(me_row, 1)] = jnp.sum(flat * flat, axis=0, keepdims=True)[None]
        square_sends = copies(
            squares.at[slot, me_row], squares.at[slot, me_row],
            lambda step: square_send.at[step], square_recv.at[slot, me_row],
            [(peer, me_col) for peer in row_peers],
        )
        for copy in square_sends:
            copy.start()
    last = LEVELS % 2
    for peer in row_peers:
        arrival(squares.at[last, peer], square_recv.at[last, peer]).wait()
    mean_square = total_square(last)
    logs_ref[LEVELS - 1 : LEVELS] = 0.5 * jnp.log(mean_square)
    sums_ref[...] = sums_ref[...] + raw[me_col] * lax.rsqrt(mean_square)
    for copy in part_sends + square_sends + depth_sends:
        copy.wait_send()


def inner_size(total):
    return max(size for size in range(1, total + 1) if total % size == 0 and size * size <= total)


def levels(dense, depth, source_ids, row_total, col_total):
    piece_tiles, width = depth.shape
    piece = piece_tiles * TILE
    inner = inner_size(row_total)
    vmem = pl.BlockSpec(memory_space=pltpu.VMEM)
    dma = pltpu.SemaphoreType.DMA
    return pl.pallas_call(
        functools.partial(level_kernel, row_total, col_total, inner),
        out_shape=(
            jax.ShapeDtypeStruct((piece, width), jnp.float32),
            jax.ShapeDtypeStruct((LEVELS, width), jnp.float32),
        ),
        in_specs=[pl.BlockSpec(memory_space=pl.ANY), vmem, vmem],
        out_specs=(vmem, vmem),
        scratch_shapes=[
            pltpu.VMEM(dense.shape, dense.dtype),
            pltpu.SemaphoreType.DMA,
            pltpu.VMEM((2, row_total, piece, width), jnp.bfloat16),
            pltpu.VMEM((2, col_total, col_total * piece, width), jnp.float32),
            pltpu.VMEM((2, row_total, 1, width), jnp.float32),
            pltpu.VMEM((col_total, piece, width), jnp.float32),
            pltpu.VMEM((col_total, piece_tiles, width), jnp.int32),
            dma((2, row_total)),
            dma((2, row_total, 2)),
            dma((col_total,)),
            dma((2, col_total)),
            dma((row_total,)),
            dma((2, row_total)),
            dma((col_total,)),
            dma((col_total,)),
        ],
        compiler_params=pltpu.CompilerParams(
            collective_id=0, has_side_effects=True, vmem_limit_bytes=56 * 1024 * 1024
        ),
        name="levels",
    )(dense, depth, source_ids)


def finish_kernel(sums_in, logs_in, sums_out, logs_out):
    sums_out[...] = sums_in[...]
    logs_out[...] = logs_in[...]


def finish(sums, logs):
    vmem = pl.BlockSpec(memory_space=pltpu.VMEM)
    return pl.pallas_call(
        finish_kernel,
        out_shape=(jax.ShapeDtypeStruct(sums.shape, sums.dtype), jax.ShapeDtypeStruct(logs.shape, logs.dtype)),
        in_specs=[vmem, vmem],
        out_specs=(vmem, vmem),
        name="finish",
    )(sums, logs)


def local(adj_tiles, tile_rows, tile_cols, tile_count, tile_depth, source_ids):
    row_total, col_total = lax.axis_size("row"), lax.axis_size("col")
    piece_tiles, width = tile_depth.shape
    dense = build(
        adj_tiles[0, 0], tile_rows[0, 0], tile_cols[0, 0], tile_count[0], col_total * piece_tiles, row_total * piece_tiles
    )
    return finish(*levels(dense, tile_depth, source_ids.reshape(1, width), row_total, col_total))


def solution(mesh):
    in_specs = (
        P("row", "col", None, None, None),
        P("row", "col", None),
        P("row", "col", None),
        P("row", "col"),
        P(("row", "col"), None),
        P(),
    )
    out_specs = (P(("row", "col"), None), P())
    return jax.shard_map(local, mesh=mesh, in_specs=in_specs, out_specs=out_specs, check_vma=False)
```
